128 devices in a mesh: gx: 4 (over x), gy: 2 (over z_hi), gz: 16 (over y, z_lo, core).
Axes of the slice: x: 4, y: 4, z: 4 (z_hi: 2, z_lo: 2; z = z_hi * 2 + z_lo), core: 2. Of those that a mesh axis runs over, the one named last changes fastest.
Arguments:
- points: float32 [3, 524288], P(None, ('gx', 'gy', 'gz')), may hold values from 0 to 1
- charges: bfloat16 [8, 524288], P(None, ('gx', 'gy', 'gz')), may hold values from -6 to 6
- arrival_order: int32 [128, 4096], P(('gx', 'gy', 'gz')), may hold values from 0 to 4095, each once within a row
- counts: int32 [128], P(('gx', 'gy', 'gz')), may hold values from 1 to 4096, 393216 in all
- basis_rows: bfloat16 [7, 524288, 128], P(None, ('gx', 'gy', 'gz')), may hold values from -6 to 6
- skeletons: float32 [3, 256, 128], replicated, may hold values from 0 to 1
Outputs:
- result: float32 [8, 524288], P(None, ('gx', 'gy', 'gz'))
The draws below stay inside these ranges and needn't reach their ends.
Inputs may be any that keep to these rules, and one draw needn't show every extreme that they name: `arrival_order`: each row is a permutation of 0 to 4095. The counts sum to 393216, and some leaf is full.
All inputs are finite; a program needn't handle non-finite values.
Results may differ from the reference program's by a relative error of at most 0.0046.
Values sent between devices are 32-bit elements; how exact they have to be, the bound alone decides.
No kernel may reach another device: no remote copies, remote signals or barrier semaphores. Data moves between devices by JAX's collectives and lax.ppermute only.
A program may use at most 64 MiB of HBM per device.

```python
import math
import jax
import jax.numpy as jnp
import numpy as np
from jax import lax

LEAF = 4096
RANK = 128
NRHS = 8
LEVELS = 7
NPTS = 524288
NODES = 256
DEVICES = 128


def steps_of(key, extent, pieces, least, high):
    factor_of, own = 1.0, jax.random.fold_in(key, 6)
    for dim, parts in pieces:
        draws = jnp.exp(jax.random.uniform(jax.random.fold_in(own, dim), (parts,), jnp.float32, least / len(pieces), high / len(pieces)))
        factor_of = factor_of * jnp.repeat(draws, extent[dim] // parts).reshape([-1 if axis == dim else 1 for axis in range(len(extent))])
    return factor_of


def split_up(amount, total, bound, lean):
    weights = [(1 << 20) // math.isqrt(rank ** lean) + 1 for rank in range(2, amount + 1)]
    rest, holding = total - bound - (amount - 1), [1] * (amount - 1)
    while rest > 0:
        movable = [i for i in range(amount - 1) if holding[i] < bound]
        whole, remaining = sum([weights[i] for i in movable]), rest
        for i in movable:
            more = min(bound - holding[i], max(1, remaining * weights[i] // whole), rest)
            holding[i] = holding[i] + more
            rest = rest - more
    return np.array([bound] + holding)


def uneven_parts(stream_key, count, total, reach, skew):
    if count == 2:
        one = jax.random.randint(stream_key, (), max(1, total - reach), min(reach, total - 1) + 1)
        return jnp.stack([one, total - one])
    lengths = jnp.asarray(split_up(count, total, reach, skew), jnp.int32)
    couples = (count - 1) // 2
    giver, taker = lengths[1:1 + 2 * couples:2], lengths[2:2 + 2 * couples:2]
    margin = jnp.minimum(giver - 1, reach - taker)
    shifted = jax.random.randint(jax.random.fold_in(stream_key, 1), (couples,), 0, 1 << 20) % (margin + 1)
    lengths = lengths.at[1:1 + 2 * couples:2].set(giver - shifted).at[2:2 + 2 * couples:2].set(taker + shifted)
    return lengths[jax.random.permutation(jax.random.fold_in(stream_key, 2), count)]


def noise(own_key, dims, spread, limit, split=(), kind=jnp.bfloat16):
    values = jax.random.normal(own_key, dims, jnp.float32) * spread
    if len(split) > 0:
        values = steps_of(own_key, dims, split, -0.22, 0.18) * values
    return jnp.clip(values, min=-limit, max=limit).astype(kind)


def setup_inputs(seed: int = 0) -> dict:
    splits = jax.random.split(jax.random.key(seed), 7)
    points = jnp.clip(1.0 * jax.random.uniform(splits[0], (3, NPTS), jnp.float32) ** steps_of(splits[0], (3, NPTS), ((1, 128),), -0.2, 0.2), 0.0, 1.0)
    charges = noise(splits[1], (NRHS, NPTS), 1.0, 6.0, ((1, 128),))
    arrival_order = jax.vmap(lambda own: jax.random.permutation(own, LEAF))(jax.random.split(splits[2], DEVICES)).reshape((DEVICES, LEAF)).astype(jnp.int32)
    counts = uneven_parts(splits[3], DEVICES, DEVICES * LEAF * 3 // 4, LEAF, 1).astype(jnp.int32)
    basis_rows = noise(splits[4], (LEVELS, NPTS, RANK), 1.0, 6.0, ((1, 128),))
    skeletons = jnp.clip(jax.random.uniform(splits[5], (3, NODES, RANK), jnp.float32, 0.0, 1.0), 0.0, 1.0)
    return dict(points=points, charges=charges, arrival_order=arrival_order, counts=counts, basis_rows=basis_rows, skeletons=skeletons)


kernel_width = 0.1
dense_gain = 4.0
expand_gain = 0.25

def squared_gap(left_pts, right_pts):
    gap_a = left_pts[0] - right_pts[0]
    gap_b = left_pts[1] - right_pts[1]
    gap_c = left_pts[2] - right_pts[2]
    return gap_a * gap_a + gap_b * gap_b + gap_c * gap_c

def reference(points, charges, arrival_order, counts, basis_rows, skeletons):
    device_count = DEVICES
    levels = LEVELS
    leaf_size = LEAF
    rank_size = RANK
    coords = jnp.transpose(points.reshape(3, device_count, leaf_size), (1, 0, 2))
    charge_grid = jnp.transpose(charges.reshape(NRHS, device_count, leaf_size), (1, 0, 2))
    tree_charges = jnp.take_along_axis(charge_grid, arrival_order[:, None, :], axis=2)
    alive_mask = jnp.arange(leaf_size, dtype=jnp.int32)[None, :] < counts[:, None]
    live_charges = jnp.where(alive_mask[:, None, :], tree_charges, jnp.zeros_like(tree_charges))
    basis_grid = jnp.transpose(basis_rows.reshape(levels, device_count, leaf_size, rank_size), (1, 0, 2, 3))
    level_scale = jnp.array([2.0 ** (-0.5 * height) / math.sqrt(leaf_size) for height in range(levels)], jnp.float32)

    def project(inputs):
        live_d, basis_d = inputs
        return jnp.einsum('kp,lpr->lkr', live_d.astype(jnp.float32), basis_d.astype(jnp.float32)) * level_scale[:, None, None]
    projection = lax.map(project, (live_charges, basis_grid))
    sibling_levels = []
    for height in range(levels):
        group_span = 2 ** height
        node_sums = projection[:, height].reshape(device_count // group_span, group_span, NRHS, rank_size).sum(axis=1)
        swapped = node_sums.reshape(-1, 2, NRHS, rank_size)[:, ::-1].reshape(device_count // group_span, NRHS, rank_size)
        sibling_levels.append(jnp.repeat(swapped, group_span, axis=0))
    sibling = jnp.stack(sibling_levels, axis=1)
    node_ids = jnp.right_shift(device_count + jnp.arange(device_count, dtype=jnp.int32)[:, None], jnp.arange(levels, dtype=jnp.int32)[None, :])

    def finish(inputs):
        sibling_d, node_d, coords_d, live_d, basis_d, alive_d = inputs
        own_pts = jnp.take(skeletons, node_d, axis=1)
        far_pts = jnp.take(skeletons, jnp.bitwise_xor(node_d, 1), axis=1)
        distance = squared_gap(far_pts[:, :, :, None], own_pts[:, :, None, :])
        coupling = jnp.exp(-distance / kernel_width).astype(jnp.bfloat16)
        sibling_rounded = sibling_d.astype(jnp.bfloat16)
        coupled = jnp.einsum('lkc,lca->lka', sibling_rounded.astype(jnp.float32), coupling.astype(jnp.float32)).astype(jnp.bfloat16)
        far_field = jnp.einsum('lka,lpa->kp', coupled.astype(jnp.float32), basis_d.astype(jnp.float32)) * (expand_gain / math.sqrt(rank_size))
        gaps = squared_gap(coords_d[:, :, None], coords_d[:, None, :])
        kernel = jnp.exp(-gaps / kernel_width).astype(jnp.bfloat16)
        near_field = jnp.dot(live_d, kernel, preferred_element_type=jnp.float32)
        total = dense_gain / math.sqrt(leaf_size) * near_field + far_field
        return jnp.where(alive_d[None, :], total, jnp.zeros_like(total))
    result = lax.map(finish, (sibling, node_ids, coords, live_charges, basis_grid, alive_mask))
    return jnp.transpose(result, (1, 0, 2)).reshape(NRHS, device_count * leaf_size)
```

```python
import math

import jax
import jax.numpy as jnp
from jax import lax
from jax.experimental import pallas as pl
from jax.experimental.pallas import tpu as pltpu
from jax.sharding import PartitionSpec as P

kernel_width = 0.1
dense_gain = 4.0
expand_gain = 0.25
axes = ("gx", "gy", "gz")
log2_rate = math.log2(math.e) / kernel_width


def device_index():
    size_y = lax.axis_size("gy")
    size_z = lax.axis_size("gz")
    return (lax.axis_index("gx") * size_y + lax.axis_index("gy")) * size_z + lax.axis_index("gz")


def head_kernel(scal_ref, order_ref, charges_ref, basis_ref, live_ref, send_ref, table_ref, acc_ref):
    step = pl.program_id(0)
    levels, rows, rank = basis_ref.shape
    rhs, leaf = charges_ref.shape
    high = leaf // 128

    @pl.when(step == 0)
    def _():
        wide = charges_ref[...].astype(jnp.float32)
        table_ref[...] = jnp.concatenate(
            [wide[:, h * 128 : (h + 1) * 128] for h in range(high)], axis=0
        ).astype(jnp.bfloat16)
        acc_ref[...] = jnp.zeros_like(acc_ref)

    order = order_ref[...]
    low_part = jnp.bitwise_and(order, 127)
    high_part = jnp.right_shift(order, 7)
    lane_of = lax.broadcasted_iota(jnp.int32, (128, rows), 0)
    one_hot = jnp.where(lane_of == low_part, 1.0, 0.0).astype(jnp.bfloat16)
    spread = jnp.dot(table_ref[...], one_hot, preferred_element_type=jnp.float32)
    high_part = jnp.broadcast_to(high_part, (rhs, rows))
    picked = jnp.zeros((rhs, rows), jnp.float32)
    for h in range(high):
        picked = jnp.where(high_part == h, spread[h * rhs : (h + 1) * rhs], picked)
    slot = lax.broadcasted_iota(jnp.int32, (rhs, rows), 1) + step * rows
    live = jnp.where(slot < scal_ref[0], picked, 0.0).astype(jnp.bfloat16)
    live_ref[...] = live
    basis = jnp.concatenate([basis_ref[l] for l in range(levels)], axis=1)
    acc_ref[...] += jnp.dot(live, basis, preferred_element_type=jnp.float32)

    @pl.when(step == pl.num_programs(0) - 1)
    def _():
        own = scal_ref[1]
        for l in range(levels):
            scale = 2.0 ** (-0.5 * l) / math.sqrt(leaf)
            block = acc_ref[:, l * rank : (l + 1) * rank] * scale
            first = jnp.bitwise_xor(own >> l, 1) << l
            for i in range(1 << l):
                send_ref[first + i] = block
        send_ref[own] = jnp.zeros((rhs, rank), jnp.float32)


def head(scal, order, charges, basis):
    levels, leaf, rank = basis.shape
    rhs = charges.shape[0]
    rows = min(512, leaf)
    return pl.pallas_call(
        head_kernel,
        grid=(leaf // rows,),
        in_specs=[
            pl.BlockSpec(memory_space=pltpu.SMEM),
            pl.BlockSpec((1, rows), lambda i: (0, i)),
            pl.BlockSpec((rhs, leaf), lambda i: (0, 0)),
            pl.BlockSpec((levels, rows, rank), lambda i: (0, i, 0)),
        ],
        out_specs=[
            pl.BlockSpec((rhs, rows), lambda i: (0, i)),
            pl.BlockSpec((1 << levels, rhs, rank), lambda i: (0, 0, 0)),
        ],
        out_shape=[
            jax.ShapeDtypeStruct((rhs, leaf), jnp.bfloat16),
            jax.ShapeDtypeStruct((1 << levels, rhs, rank), jnp.float32),
        ],
        scratch_shapes=[
            pltpu.VMEM((leaf // 128 * rhs, 128), jnp.bfloat16),
            pltpu.VMEM((rhs, levels * rank), jnp.float32),
        ],
        compiler_params=pltpu.CompilerParams(vmem_limit_bytes=24 << 20),
        name="head",
    )(scal, order, charges, basis)


def bf16_pieces(x):
    pieces = []
    for _ in range(3):
        piece = x.astype(jnp.bfloat16).astype(jnp.float32)
        pieces.append(piece)
        x = x - piece
    return pieces


def near_kernel(scal_ref, points_ref, live_ref, skel_ref, near_ref, coup_ref, tall_ref, wide_ref, spare_ref):
    step = pl.program_id(0)
    rhs, leaf = live_ref.shape
    columns = near_ref.shape[1]
    rows = min(512, leaf)

    @pl.when(step == 0)
    def _():
        scaled = (points_ref[...] - 0.5) * math.sqrt(2.0 * log2_rate)
        high, mid, low = bf16_pieces(scaled)
        norm = jnp.sum(scaled * scaled, axis=0, keepdims=True) * -0.5
        norms = jnp.concatenate(bf16_pieces(norm), axis=0)
        ones = jnp.ones_like(norms)
        spare_ref[...] = jnp.zeros_like(spare_ref)
        for at, piece in ((0, high), (3, norms), (8, mid), (11, ones), (16, low), (24, high), (32, mid), (40, high)):
            spare_ref[at : at + 3, :] = piece
        for b in range(leaf // 128):
            tall_ref[b * 128 : (b + 1) * 128, :] = spare_ref[:, b * 128 : (b + 1) * 128].T.astype(jnp.bfloat16)
        for at, piece in ((0, high), (3, ones), (8, high), (11, norms), (16, high), (24, mid), (32, mid), (40, low)):
            spare_ref[at : at + 3, :] = piece
        wide_ref[...] = spare_ref[...].astype(jnp.bfloat16)

        own = scal_ref[1]
        devices = 1 << coup_ref.shape[0]
        for l in range(coup_ref.shape[0]):
            node = (devices + own) >> l
            gap = None
            for axis in range(3):
                mine = skel_ref[axis, pl.ds(node, 1), :]
                other = skel_ref[axis, pl.ds(jnp.bitwise_xor(node, 1), 1), :]
                other = jnp.broadcast_to(other, (other.shape[1], other.shape[1])).T
                diff = other - mine
                gap = diff * diff if gap is None else gap + diff * diff
            coup_ref[l] = jnp.exp2(gap * -log2_rate).astype(jnp.bfloat16)

    column = wide_ref[:, pl.ds(pl.multiple_of(step * columns, 128), columns)]
    total = jnp.zeros((rhs, columns), jnp.float32)
    for at in range(0, leaf, rows):
        power = jnp.dot(tall_ref[at : at + rows, :], column, preferred_element_type=jnp.float32)
        kernel = jnp.exp2(power).astype(jnp.bfloat16)
        total += jnp.dot(live_ref[:, at : at + rows], kernel, preferred_element_type=jnp.float32)
    near_ref[...] = total


def near(scal, points, live, skeletons, levels):
    rhs, leaf = live.shape
    rank = skeletons.shape[2]
    columns = min(256, leaf)
    return pl.pallas_call(
        near_kernel,
        grid=(leaf // columns,),
        in_specs=[
            pl.BlockSpec(memory_space=pltpu.SMEM),
            pl.BlockSpec((3, leaf), lambda i: (0, 0)),
            pl.BlockSpec((rhs, leaf), lambda i: (0, 0)),
            pl.BlockSpec(skeletons.shape, lambda i: (0, 0, 0)),
        ],
        out_specs=[
            pl.BlockSpec((rhs, columns), lambda i: (0, i)),
            pl.BlockSpec((levels, rank, rank), lambda i: (0, 0, 0)),
        ],
        out_shape=[
            jax.ShapeDtypeStruct((rhs, leaf), jnp.float32),
            jax.ShapeDtypeStruct((levels, rank, rank), jnp.bfloat16),
        ],
        scratch_shapes=[
            pltpu.VMEM((leaf, 48), jnp.bfloat16),
            pltpu.VMEM((48, leaf), jnp.bfloat16),
            pltpu.VMEM((48, leaf), jnp.float32),
        ],
        compiler_params=pltpu.CompilerParams(vmem_limit_bytes=24 << 20),
        cost_estimate=pl.CostEstimate(flops=4 << 30, bytes_accessed=1 << 20, transcendentals=leaf * leaf),
        name="near",
    )(scal, points, live, skeletons)


def tail_kernel(scal_ref, got_ref, coup_ref, near_ref, basis_ref, out_ref, coupled_ref):
    step = pl.program_id(0)
    levels, rows, rank = basis_ref.shape
    rhs = near_ref.shape[0]
    leaf = rows * pl.num_programs(0)

    @pl.when(step == 0)
    def _():
        own = scal_ref[1]
        for l in range(levels):
            first = jnp.bitwise_xor(own >> l, 1) << l
            sums = [got_ref[first + i] for i in range(1 << l)]
            while len(sums) > 1:
                sums = [a + b for a, b in zip(sums[::2], sums[1::2])]
            coupled = jnp.dot(sums[0].astype(jnp.bfloat16), coup_ref[l], preferred_element_type=jnp.float32)
            coupled_ref[:, l * rank : (l + 1) * rank] = coupled.astype(jnp.bfloat16)

    basis = jnp.concatenate([basis_ref[l] for l in range(levels)], axis=1)
    far = lax.dot_general(
        coupled_ref[...], basis, (((1,), (1,)), ((), ())), preferred_element_type=jnp.float32
    )
    total = dense_gain / math.sqrt(leaf) * near_ref[...] + far * (expand_gain / math.sqrt(rank))
    slot = lax.broadcasted_iota(jnp.int32, (rhs, rows), 1) + step * rows
    out_ref[...] = jnp.where(slot < scal_ref[0], total, 0.0)


def tail(scal, got, coup, near_field, basis):
    levels, leaf, rank = basis.shape
    rhs = near_field.shape[0]
    rows = min(512, leaf)
    return pl.pallas_call(
        tail_kernel,
        grid=(leaf // rows,),
        in_specs=[
            pl.BlockSpec(memory_space=pltpu.SMEM),
            pl.BlockSpec(got.shape, lambda i: (0, 0, 0)),
            pl.BlockSpec(coup.shape, lambda i: (0, 0, 0)),
            pl.BlockSpec((rhs, rows), lambda i: (0, i)),
            pl.BlockSpec((levels, rows, rank), lambda i: (0, i, 0)),
        ],
        out_specs=pl.BlockSpec((rhs, rows), lambda i: (0, i)),
        out_shape=jax.ShapeDtypeStruct((rhs, leaf), jnp.float32),
        scratch_shapes=[pltpu.VMEM((rhs, levels * rank), jnp.bfloat16)],
        compiler_params=pltpu.CompilerParams(vmem_limit_bytes=24 << 20),
        name="tail",
    )(scal, got, coup, near_field, basis)


def per_device(points, charges, arrival_order, counts, basis_rows, skeletons):
    scal = jnp.stack([counts[0], device_index()])
    live, send = head(scal, arrival_order, charges, basis_rows)
    got = lax.all_to_all(send, axes, 0, 0, tiled=True)
    near_field, coup = near(scal, points, live, skeletons, basis_rows.shape[0])
    return tail(scal, got, coup, near_field, basis_rows)


def solution(mesh):
    placed = (
        P(None, axes),
        P(None, axes),
        P(axes, None),
        P(axes),
        P(None, axes, None),
        P(),
    )
    return jax.shard_map(
        per_device,
        mesh=mesh,
        in_specs=placed,
        out_specs=P(None, axes),
        check_vma=False,
    )
```

```python
import math

import jax
import jax.numpy as jnp
from jax import lax
from jax.experimental import pallas as pl
from jax.experimental.pallas import tpu as pltpu
from jax.sharding import PartitionSpec as P

kernel_width = 0.1
dense_gain = 4.0
expand_gain = 0.25
axes = ("gx", "gy", "gz")
log2_rate = math.log2(math.e) / kernel_width


def in_hbm(x):
    return pltpu.with_memory_space_constraint(x, pltpu.HBM)


def device_index():
    size_y = lax.axis_size("gy")
    size_z = lax.axis_size("gz")
    return (lax.axis_index("gx") * size_y + lax.axis_index("gy")) * size_z + lax.axis_index("gz")


def bf16_pieces(x):
    pieces = []
    for _ in range(3):
        piece = x.astype(jnp.bfloat16).astype(jnp.float32)
        pieces.append(piece)
        x = x - piece
    return pieces


def features(points_ref, tall_ref, wide_ref, spare_ref):
    leaf = points_ref.shape[1]
    spare_ref[...] = jnp.zeros_like(spare_ref)
    spare_ref[0:3, :] = (points_ref[...] - 0.5) * math.sqrt(2.0 * log2_rate)
    scaled = spare_ref[...]
    high, mid, _ = bf16_pieces(scaled)
    norm = jnp.sum(scaled * scaled, axis=0, keepdims=True) * -0.5
    norms = bf16_pieces(jnp.broadcast_to(norm, scaled.shape))
    row = lax.broadcasted_iota(jnp.int32, scaled.shape, 0)
    place = jnp.where(row == 3, norms[0], jnp.where(row == 4, norms[1], jnp.where(row == 5, norms[2], 0.0)))
    ones = jnp.where((row >= 3) & (row < 6), 1.0, 0.0)
    axis = row < 3
    wide = [jnp.where(axis, high, ones), jnp.where(axis, high, place), mid, mid]
    tall = [jnp.where(axis, high, place), jnp.where(axis, mid, ones), high, mid]
    wide_ref[...] = jnp.concatenate(wide, axis=0).astype(jnp.bfloat16)
    tall = jnp.concatenate(tall, axis=0)
    for b in range(leaf // 128):
        tall_ref[b * 128 : (b + 1) * 128, :] = tall[:, b * 128 : (b + 1) * 128].T.astype(jnp.bfloat16)


def head_kernel(
    scal_ref, order_hbm, charges_hbm, points_hbm, basis_hbm,
    live_ref, send_ref, tall_ref, wide_ref,
    basis_ref, order_ref, charges_ref, points_ref, table_ref, acc_ref, spare_ref, sems,
):
    levels, leaf, rank = basis_ref.shape
    rhs = charges_ref.shape[0]
    high = leaf // 128
    rows = min(512, leaf)
    steps = leaf // rows
    small = [
        pltpu.make_async_copy(charges_hbm, charges_ref, sems.at[steps]),
        pltpu.make_async_copy(order_hbm, order_ref, sems.at[steps + 1]),
        pltpu.make_async_copy(points_hbm, points_ref, sems.at[steps + 2]),
    ]
    large = [
        pltpu.make_async_copy(
            basis_hbm.at[:, pl.ds(s * rows, rows), :], basis_ref.at[:, pl.ds(s * rows, rows), :], sems.at[s]
        )
        for s in range(steps)
    ]
    for copy in small + large:
        copy.start()
    small[2].wait()
    features(points_ref, tall_ref, wide_ref, spare_ref)
    small[0].wait()
    small[1].wait()
    wide = charges_ref[...].astype(jnp.float32)
    table_ref[...] = jnp.concatenate(
        [wide[:, h * 128 : (h + 1) * 128] for h in range(high)], axis=0
    ).astype(jnp.bfloat16)
    acc_ref[...] = jnp.zeros_like(acc_ref)
    for s in range(steps):
        order = order_ref[:, s * rows : (s + 1) * rows]
        low_part = jnp.bitwise_and(order, 127)
        high_part = jnp.broadcast_to(jnp.right_shift(order, 7), (rhs, rows))
        lane_of = lax.broadcasted_iota(jnp.int32, (128, rows), 0)
        one_hot = jnp.where(lane_of == low_part, 1.0, 0.0).astype(jnp.bfloat16)
        spread = jnp.dot(table_ref[...], one_hot, preferred_element_type=jnp.float32)
        picked = jnp.zeros((rhs, rows), jnp.float32)
        for h in range(high):
            picked = jnp.where(high_part == h, spread[h * rhs : (h + 1) * rhs], picked)
        slot = lax.broadcasted_iota(jnp.int32, (rhs, rows), 1) + s * rows
        live = jnp.where(slot < scal_ref[0], picked, 0.0).astype(jnp.bfloat16)
        live_ref[:, s * rows : (s + 1) * rows] = live
    for s in range(steps):
        large[s].wait()
        live = live_ref[:, s * rows : (s + 1) * rows]
        basis = jnp.concatenate([basis_ref[l, s * rows : (s + 1) * rows, :] for l in range(levels)], axis=1)
        acc_ref[...] += jnp.dot(live, basis, preferred_element_type=jnp.float32)
    own = scal_ref[1]
    for l in range(levels):
        scale = 2.0 ** (-0.5 * l) / math.sqrt(leaf)
        block = acc_ref[:, l * rank : (l + 1) * rank] * scale
        first = jnp.bitwise_xor(own >> l, 1) << l
        for i in range(1 << l):
            send_ref[first + i] = block
    send_ref[own] = jnp.zeros((rhs, rank), jnp.float32)


def head(scal, order, charges, points, basis):
    levels, leaf, rank = basis.shape
    rhs = charges.shape[0]
    vmem = pl.BlockSpec(memory_space=pltpu.VMEM)
    hbm = pl.BlockSpec(memory_space=pltpu.HBM)
    return pl.pallas_call(
        head_kernel,
        in_specs=[pl.BlockSpec(memory_space=pltpu.SMEM), hbm, hbm, hbm, hbm],
        out_specs=[vmem, vmem, vmem, vmem],
        out_shape=[
            jax.ShapeDtypeStruct((rhs, leaf), jnp.bfloat16),
            pltpu.VMEM((1 << levels, rhs, rank), jnp.float32),
            jax.ShapeDtypeStruct((leaf, 32), jnp.bfloat16),
            jax.ShapeDtypeStruct((32, leaf), jnp.bfloat16),
        ],
        scratch_shapes=[
            pltpu.VMEM(basis.shape, basis.dtype),
            pltpu.VMEM(order.shape, order.dtype),
            pltpu.VMEM(charges.shape, charges.dtype),
            pltpu.VMEM(points.shape, points.dtype),
            pltpu.VMEM((leaf // 128 * rhs, 128), jnp.bfloat16),
            pltpu.VMEM((rhs, levels * rank), jnp.float32),
            pltpu.VMEM((8, leaf), jnp.float32),
            pltpu.SemaphoreType.DMA((leaf // min(512, leaf) + 3,)),
        ],
        compiler_params=pltpu.CompilerParams(vmem_limit_bytes=24 << 20),
        name="head",
    )(scal, *[in_hbm(x) for x in (order, charges, points, basis)])


def near_kernel(scal_ref, tall_ref, wide_ref, live_ref, skel_ref, near_ref, coup_ref):
    rhs, leaf = live_ref.shape
    columns = min(2048, leaf)
    rows = min(512, leaf)
    own = scal_ref[1]
    devices = 1 << coup_ref.shape[0]
    for l in range(coup_ref.shape[0]):
        node = (devices + own) >> l
        gap = None
        for axis in range(3):
            mine = skel_ref[axis, pl.ds(node, 1), :]
            other = skel_ref[axis, pl.ds(jnp.bitwise_xor(node, 1), 1), :]
            other = jnp.broadcast_to(other, (other.shape[1], other.shape[1])).T
            diff = other - mine
            gap = diff * diff if gap is None else gap + diff * diff
        coup_ref[l] = jnp.exp2(gap * -log2_rate).astype(jnp.bfloat16)

    def column_block(step, carry):
        first = pl.multiple_of(step * columns, 128)
        column = wide_ref[:, pl.ds(first, columns)]
        total = jnp.zeros((rhs, columns), jnp.float32)
        for at in range(0, leaf, rows):
            power = jnp.dot(tall_ref[at : at + rows, :], column, preferred_element_type=jnp.float32)
            kernel = jnp.exp2(power).astype(jnp.bfloat16)
            total += jnp.dot(live_ref[:, at : at + rows], kernel, preferred_element_type=jnp.float32)
        near_ref[:, pl.ds(first, columns)] = total
        return carry

    lax.fori_loop(0, leaf // columns, column_block, 0)


def near(scal, tall, wide, live, skeletons, levels):
    rhs, leaf = live.shape
    rank = skeletons.shape[2]
    vmem = pl.BlockSpec(memory_space=pltpu.VMEM)
    return pl.pallas_call(
        near_kernel,
        in_specs=[pl.BlockSpec(memory_space=pltpu.SMEM), vmem, vmem, vmem, vmem],
        out_specs=[vmem, vmem],
        out_shape=[
            jax.ShapeDtypeStruct((rhs, leaf), jnp.float32),
            jax.ShapeDtypeStruct((levels, rank, rank), jnp.bfloat16),
        ],
        compiler_params=pltpu.CompilerParams(vmem_limit_bytes=24 << 20),
        cost_estimate=pl.CostEstimate(flops=4 << 30, bytes_accessed=1 << 20, transcendentals=leaf * leaf),
        name="near",
    )(scal, tall, wide, live, skeletons)


def tail_kernel(scal_ref, got_ref, coup_ref, near_ref, basis_hbm, out_ref, basis_ref, coupled_ref, sems):
    levels, leaf, rank = basis_ref.shape
    rhs = near_ref.shape[0]
    rows = min(512, leaf)
    copies = [
        pltpu.make_async_copy(
            basis_hbm.at[:, pl.ds(s * rows, rows), :], basis_ref.at[:, pl.ds(s * rows, rows), :], sems.at[s]
        )
        for s in range(leaf // rows)
    ]
    for copy in copies:
        copy.start()
    own = scal_ref[1]
    for l in range(levels):
        first = jnp.bitwise_xor(own >> l, 1) << l
        sums = [got_ref[first + i] for i in range(1 << l)]
        while len(sums) > 1:
            sums = [a + b for a, b in zip(sums[::2], sums[1::2])]
        coupled = jnp.dot(sums[0].astype(jnp.bfloat16), coup_ref[l], preferred_element_type=jnp.float32)
        coupled_ref[:, l * rank : (l + 1) * rank] = coupled.astype(jnp.bfloat16)
    for s in range(leaf // rows):
        at = s * rows
        copies[s].wait()
        basis = jnp.concatenate([basis_ref[l, at : at + rows, :] for l in range(levels)], axis=1)
        far = lax.dot_general(
            coupled_ref[...], basis, (((1,), (1,)), ((), ())), preferred_element_type=jnp.float32
        )
        field = dense_gain / math.sqrt(leaf) * near_ref[:, at : at + rows] + far * (expand_gain / math.sqrt(rank))
        slot = lax.broadcasted_iota(jnp.int32, (rhs, rows), 1) + at
        out_ref[:, at : at + rows] = jnp.where(slot < scal_ref[0], field, 0.0)


def tail(scal, got, coup, near_field, basis):
    levels, leaf, rank = basis.shape
    rhs = near_field.shape[0]
    rows = min(512, leaf)
    vmem = pl.BlockSpec(memory_space=pltpu.VMEM)
    return pl.pallas_call(
        tail_kernel,
        in_specs=[pl.BlockSpec(memory_space=pltpu.SMEM), vmem, vmem, vmem, pl.BlockSpec(memory_space=pltpu.HBM)],
        out_specs=vmem,
        out_shape=jax.ShapeDtypeStruct((rhs, leaf), jnp.float32),
        scratch_shapes=[
            pltpu.VMEM(basis.shape, basis.dtype),
            pltpu.VMEM((rhs, levels * rank), jnp.bfloat16),
            pltpu.SemaphoreType.DMA((leaf // rows,)),
        ],
        compiler_params=pltpu.CompilerParams(vmem_limit_bytes=24 << 20),
        name="tail",
    )(scal, got, coup, near_field, in_hbm(basis))


def per_device(points, charges, arrival_order, counts, basis_rows, skeletons):
    scal = jnp.stack([counts[0], device_index()])
    live, send, tall, wide = head(scal, arrival_order, charges, points, basis_rows)
    got = lax.all_to_all(send, axes, 0, 0, tiled=True)
    near_field, coup = near(scal, tall, wide, live, skeletons, basis_rows.shape[0])
    return tail(scal, got, coup, near_field, basis_rows)


def solution(mesh):
    placed = (
        P(None, axes),
        P(None, axes),
        P(axes, None),
        P(axes),
        P(None, axes, None),
        P(),
    )
    return jax.shard_map(
        per_device,
        mesh=mesh,
        in_specs=placed,
        out_specs=P(None, axes),
        check_vma=False,
    )
```

```python
import math

import jax
import jax.numpy as jnp
from jax import lax
from jax.experimental import pallas as pl
from jax.experimental.pallas import tpu as pltpu
from jax.sharding import PartitionSpec as P

kernel_width = 0.1
dense_gain = 4.0
expand_gain = 0.25
axes = ("gx", "gy", "gz")
log2_rate = math.log2(math.e) / kernel_width


def in_hbm(x):
    return pltpu.with_memory_space_constraint(x, pltpu.HBM)


def device_index():
    size_y = lax.axis_size("gy")
    size_z = lax.axis_size("gz")
    return (lax.axis_index("gx") * size_y + lax.axis_index("gy")) * size_z + lax.axis_index("gz")


def bf16_pieces(x):
    pieces = []
    for _ in range(3):
        piece = x.astype(jnp.bfloat16).astype(jnp.float32)
        pieces.append(piece)
        x = x - piece
    return pieces


def features(points_ref, tall_ref, wide_ref, spare_ref):
    leaf = points_ref.shape[1]
    spare_ref[...] = jnp.zeros_like(spare_ref)
    spare_ref[0:3, :] = (points_ref[...] - 0.5) * math.sqrt(2.0 * log2_rate)
    scaled = spare_ref[...]
    high, mid, _ = bf16_pieces(scaled)
    norm = jnp.sum(scaled * scaled, axis=0, keepdims=True) * -0.5
    norms = bf16_pieces(jnp.broadcast_to(norm, scaled.shape))
    row = lax.broadcasted_iota(jnp.int32, scaled.shape, 0)
    place = jnp.where(row == 3, norms[0], jnp.where(row == 4, norms[1], jnp.where(row == 5, norms[2], 0.0)))
    ones = jnp.where((row >= 3) & (row < 6), 1.0, 0.0)
    axis = row < 3
    wide = [jnp.where(axis, high, ones), jnp.where(axis, high, place), mid, mid]
    tall = [jnp.where(axis, high, place), jnp.where(axis, mid, ones), high, mid]
    wide_ref[...] = jnp.concatenate(wide, axis=0).astype(jnp.bfloat16)
    tall = jnp.concatenate(tall, axis=0)
    side = leaf // 4
    for at in range(0, side, 128):
        quarters = [tall[:, g * side + at : g * side + at + 128] for g in range(4)]
        tall_ref[at : at + 128, :] = jnp.concatenate(quarters, axis=0).T.astype(jnp.bfloat16)


def head_kernel(
    scal_ref, order_hbm, charges_hbm, points_hbm, basis_hbm,
    live_ref, proj_ref, tall_ref, wide_ref,
    basis_ref, order_ref, charges_ref, points_ref, table_ref, acc_ref, spare_ref, sems,
):
    levels, leaf, rank = basis_ref.shape
    rhs = charges_ref.shape[0]
    high = leaf // 128
    rows = min(1024, leaf)
    steps = leaf // rows
    small = [
        pltpu.make_async_copy(charges_hbm, charges_ref, sems.at[steps]),
        pltpu.make_async_copy(order_hbm, order_ref, sems.at[steps + 1]),
        pltpu.make_async_copy(points_hbm, points_ref, sems.at[steps + 2]),
    ]
    large = [
        pltpu.make_async_copy(
            basis_hbm.at[:, pl.ds(s * rows, rows), :], basis_ref.at[:, pl.ds(s * rows, rows), :], sems.at[s]
        )
        for s in range(steps)
    ]
    for copy in small + large:
        copy.start()
    small[2].wait()
    features(points_ref, tall_ref, wide_ref, spare_ref)
    small[0].wait()
    small[1].wait()
    wide = charges_ref[...].astype(jnp.float32)
    table_ref[...] = jnp.concatenate(
        [wide[:, h * 128 : (h + 1) * 128] for h in range(high)], axis=0
    ).astype(jnp.bfloat16)
    acc_ref[...] = jnp.zeros_like(acc_ref)
    for s in range(steps):
        order = order_ref[:, s * rows : (s + 1) * rows]
        low_part = jnp.bitwise_and(order, 127)
        high_part = jnp.broadcast_to(jnp.right_shift(order, 7), (rhs, rows))
        lane_of = lax.broadcasted_iota(jnp.int32, (128, rows), 0)
        one_hot = jnp.where(lane_of == low_part, 1.0, 0.0).astype(jnp.bfloat16)
        spread = jnp.dot(table_ref[...], one_hot, preferred_element_type=jnp.float32)
        picked = jnp.zeros((rhs, rows), jnp.float32)
        for h in range(high):
            picked = jnp.where(high_part == h, spread[h * rhs : (h + 1) * rhs], picked)
        slot = lax.broadcasted_iota(jnp.int32, (rhs, rows), 1) + s * rows
        live = jnp.where(slot < scal_ref[0], picked, 0.0).astype(jnp.bfloat16)
        live_ref[:, s * rows : (s + 1) * rows] = live
    for s in range(steps):
        large[s].wait()
        live = live_ref[:, s * rows : (s + 1) * rows]
        basis = jnp.concatenate([basis_ref[l, s * rows : (s + 1) * rows, :] for l in range(levels)], axis=1)
        acc_ref[...] += jnp.dot(live, basis, preferred_element_type=jnp.float32)
    for l in range(levels):
        scale = 2.0 ** (-0.5 * l) / math.sqrt(leaf)
        proj_ref[l] = acc_ref[:, l * rank : (l + 1) * rank] * scale


def head(scal, order, charges, points, basis):
    levels, leaf, rank = basis.shape
    rhs = charges.shape[0]
    vmem = pl.BlockSpec(memory_space=pltpu.VMEM)
    hbm = pl.BlockSpec(memory_space=pltpu.HBM)
    return pl.pallas_call(
        head_kernel,
        in_specs=[pl.BlockSpec(memory_space=pltpu.SMEM), hbm, hbm, hbm, hbm],
        out_specs=[vmem, vmem, vmem, vmem],
        out_shape=[
            jax.ShapeDtypeStruct((rhs, leaf), jnp.bfloat16),
            jax.ShapeDtypeStruct((levels, rhs, rank), jnp.float32),
            jax.ShapeDtypeStruct((leaf // 4, 128), jnp.bfloat16),
            jax.ShapeDtypeStruct((32, leaf), jnp.bfloat16),
        ],
        scratch_shapes=[
            pltpu.VMEM(basis.shape, basis.dtype),
            pltpu.VMEM(order.shape, order.dtype),
            pltpu.VMEM(charges.shape, charges.dtype),
            pltpu.VMEM(points.shape, points.dtype),
            pltpu.VMEM((leaf // 128 * rhs, 128), jnp.bfloat16),
            pltpu.VMEM((rhs, levels * rank), jnp.float32),
            pltpu.VMEM((8, leaf), jnp.float32),
            pltpu.SemaphoreType.DMA((leaf // min(1024, leaf) + 3,)),
        ],
        compiler_params=pltpu.CompilerParams(vmem_limit_bytes=24 << 20),
        name="head",
    )(scal, *[in_hbm(x) for x in (order, charges, points, basis)])


def near_blocks(tall_ref, wide_ref, live_ref, near_ref):
    side = live_ref.shape[1] // 4
    near_ref[...] = jnp.zeros_like(near_ref)
    for row in range(4):
        for col in range(row, 4):
            own = slice(row * side, (row + 1) * side)
            other = slice(col * side, (col + 1) * side)
            column = [wide_ref[:, other] if g == row else jnp.zeros((32, side), jnp.bfloat16) for g in range(4)]
            power = jnp.dot(tall_ref[...], jnp.concatenate(column, axis=0), preferred_element_type=jnp.float32)
            kernel = jnp.exp2(power).astype(jnp.bfloat16)
            near_ref[:, other] += jnp.dot(live_ref[:, own], kernel, preferred_element_type=jnp.float32)
            if row != col:
                near_ref[:, own] += lax.dot_general(
                    live_ref[:, other], kernel, (((1,), (1,)), ((), ())), preferred_element_type=jnp.float32
                )


def couple_kernel(scal_ref, live_hbm, skel_ref, coup_ref):
    own = scal_ref[1]
    devices = 1 << coup_ref.shape[0]
    for l in range(coup_ref.shape[0]):
        node = (devices + own) >> l
        gap = None
        for axis in range(3):
            mine = skel_ref[axis, pl.ds(node, 1), :]
            other = skel_ref[axis, pl.ds(jnp.bitwise_xor(node, 1), 1), :]
            other = jnp.broadcast_to(other, (other.shape[1], other.shape[1])).T
            diff = other - mine
            gap = diff * diff if gap is None else gap + diff * diff
        coup_ref[l] = jnp.exp2(gap * -log2_rate).astype(jnp.bfloat16)


def couple(scal, live, skeletons, levels):
    rank = skeletons.shape[2]
    vmem = pl.BlockSpec(memory_space=pltpu.VMEM)
    return pl.pallas_call(
        couple_kernel,
        in_specs=[pl.BlockSpec(memory_space=pltpu.SMEM), pl.BlockSpec(memory_space=pl.ANY), vmem],
        out_specs=vmem,
        out_shape=jax.ShapeDtypeStruct((levels, rank, rank), jnp.bfloat16),
        compiler_params=pltpu.CompilerParams(vmem_limit_bytes=8 << 20),
        cost_estimate=pl.CostEstimate(flops=1 << 20, bytes_accessed=1 << 19, transcendentals=1 << 17),
        name="couple",
    )(scal, live, skeletons)


def pack_kernel(scal_ref, mine_ref, other_ref, send_ref):
    own = scal_ref[1] >> 1
    levels = mine_ref.shape[0]
    for l in range(1, levels):
        block = mine_ref[l] + other_ref[l]
        first = jnp.bitwise_xor(own >> (l - 1), 1) << (l - 1)
        for i in range(1 << (l - 1)):
            send_ref[first + i] = block
    send_ref[own] = jnp.zeros(mine_ref.shape[1:], jnp.float32)


def pack(scal, mine, other):
    vmem = pl.BlockSpec(memory_space=pltpu.VMEM)
    return pl.pallas_call(
        pack_kernel,
        in_specs=[pl.BlockSpec(memory_space=pltpu.SMEM), vmem, vmem],
        out_specs=vmem,
        out_shape=jax.ShapeDtypeStruct((1 << (mine.shape[0] - 1), *mine.shape[1:]), jnp.float32),
        compiler_params=pltpu.CompilerParams(vmem_limit_bytes=8 << 20),
        name="pack",
    )(scal, mine, other)


def near_kernel(tall_ref, wide_ref, live_ref, send_hbm, basis_hbm, near_ref, kept_ref, sem):
    held = kept_ref.shape[0]
    copy = pltpu.make_async_copy(basis_hbm.at[pl.ds(basis_hbm.shape[0] - held, held)], kept_ref, sem)
    copy.start()
    near_blocks(tall_ref, wide_ref, live_ref, near_ref)
    copy.wait()


def near(tall, wide, live, send, basis, held):
    rhs, leaf = live.shape
    vmem = pl.BlockSpec(memory_space=pltpu.VMEM)
    return pl.pallas_call(
        near_kernel,
        in_specs=[vmem, vmem, vmem, pl.BlockSpec(memory_space=pl.ANY), pl.BlockSpec(memory_space=pltpu.HBM)],
        out_specs=[vmem, vmem],
        out_shape=[
            jax.ShapeDtypeStruct((rhs, leaf), jnp.float32),
            pltpu.VMEM((held, *basis.shape[1:]), basis.dtype),
        ],
        scratch_shapes=[pltpu.SemaphoreType.DMA(())],
        compiler_params=pltpu.CompilerParams(vmem_limit_bytes=24 << 20),
        cost_estimate=pl.CostEstimate(flops=4 << 30, bytes_accessed=1 << 20, transcendentals=leaf * leaf),
        name="near",
    )(tall, wide, live, send, in_hbm(basis))


def tail_kernel(
    scal_ref, other_ref, got_ref, coup_ref, near_ref, kept_ref, basis_hbm, out_ref, basis_ref, coupled_ref, sems
):
    fetched, leaf, rank = basis_ref.shape
    levels = fetched + kept_ref.shape[0]
    rhs = near_ref.shape[0]
    copies = [pltpu.make_async_copy(basis_hbm.at[l], basis_ref.at[l], sems.at[l]) for l in range(fetched)]
    for copy in copies:
        copy.start()
    own = scal_ref[1] >> 1
    for l in range(levels):
        if l == 0:
            sums = [other_ref[0]]
        else:
            first = jnp.bitwise_xor(own >> (l - 1), 1) << (l - 1)
            sums = [got_ref[first + i] for i in range(1 << (l - 1))]
        while len(sums) > 1:
            sums = [a + b for a, b in zip(sums[::2], sums[1::2])]
        coupled = jnp.dot(sums[0].astype(jnp.bfloat16), coup_ref[l], preferred_element_type=jnp.float32)
        coupled_ref[:, l * rank : (l + 1) * rank] = coupled.astype(jnp.bfloat16)
    out_ref[...] = near_ref[...] * (dense_gain / math.sqrt(leaf))
    parts = [range(fetched, levels)] + [range(l, min(l + 2, fetched)) for l in range(0, fetched, 2)]
    for part in parts:
        rows = []
        for l in part:
            if l < fetched:
                copies[l].wait()
            rows.append(basis_ref[l] if l < fetched else kept_ref[l - fetched])
        coupled = coupled_ref[:, part[0] * rank : (part[-1] + 1) * rank]
        far = lax.dot_general(
            coupled, jnp.concatenate(rows, axis=1), (((1,), (1,)), ((), ())), preferred_element_type=jnp.float32
        )
        out_ref[...] += far * (expand_gain / math.sqrt(rank))
    slot = lax.broadcasted_iota(jnp.int32, (rhs, leaf), 1)
    out_ref[...] = jnp.where(slot < scal_ref[0], out_ref[...], 0.0)


def tail(scal, other, got, coup, near_field, kept, basis):
    levels, leaf, rank = basis.shape
    rhs = near_field.shape[0]
    vmem = pl.BlockSpec(memory_space=pltpu.VMEM)
    return pl.pallas_call(
        tail_kernel,
        in_specs=[pl.BlockSpec(memory_space=pltpu.SMEM)] + [vmem] * 5 + [pl.BlockSpec(memory_space=pltpu.HBM)],
        out_specs=vmem,
        out_shape=jax.ShapeDtypeStruct((rhs, leaf), jnp.float32),
        scratch_shapes=[
            pltpu.VMEM((levels - kept.shape[0], leaf, rank), basis.dtype),
            pltpu.VMEM((rhs, levels * rank), jnp.bfloat16),
            pltpu.SemaphoreType.DMA((levels - kept.shape[0],)),
        ],
        compiler_params=pltpu.CompilerParams(vmem_limit_bytes=24 << 20),
        name="tail",
    )(scal, other, got, coup, near_field, kept, in_hbm(basis))


def per_device(points, charges, arrival_order, counts, basis_rows, skeletons):
    scal = jnp.stack([counts[0], device_index()])
    live, mine, tall, wide = head(scal, arrival_order, charges, points, basis_rows)
    count = 1 << basis_rows.shape[0]
    other = lax.ppermute(mine, axes, [(d, d ^ 1) for d in range(count)])
    coup = couple(scal, live, skeletons, basis_rows.shape[0])
    send = pack(scal, mine, other)
    chips = [list(range(core, count, 2)) for core in range(2)]
    got = lax.all_to_all(send, axes, 0, 0, axis_index_groups=chips, tiled=True)
    near_field, kept = near(tall, wide, live, send, basis_rows, 2)
    return tail(scal, other, got, coup, near_field, kept, basis_rows)


def solution(mesh):
    placed = (
        P(None, axes),
        P(None, axes),
        P(axes, None),
        P(axes),
        P(None, axes, None),
        P(),
    )
    return jax.shard_map(
        per_device,
        mesh=mesh,
        in_specs=placed,
        out_specs=P(None, axes),
        check_vma=False,
    )
```
